32 devices in a mesh: grp: 2 (over y), row: 4 (over x, core), sub: 4 (over z).
Axes of the slice: x: 2, y: 2, z: 4, core: 2. Of those that a mesh axis runs over, the one named last changes fastest.
Arguments:
- residual_in: float32 [4, 2048, 2048], P('grp', ('row', 'sub')), parts along dimension 0, may hold values from -100 to 100
- direction: float32 [4, 2048, 2048], P('grp', ('row', 'sub')), parts along dimension 0, may hold values from -100 to 100
- spectrum: float32 [8192, 4096], P('grp', ('row', 'sub')), parts along dimension 0, may hold values from 0.0999 to 10.001, as said below
- noise_var: float32 [2], P('grp'), parts along dimension 0, may hold values from 0.5 to 2
Outputs:
- residual_out: float32 [4, 2048, 2048], P('grp', ('row', 'sub')), parts along dimension 0
- direction_out: float32 [4, 2048, 2048], P('grp', ('row', 'sub')), parts along dimension 0
- step_size: float32 [4], P('grp'), parts along dimension 0
The draws below stay inside these ranges and needn't reach their ends.
There are 2 independent parts, one for each index of `grp`. The reference program is written for one: setup_inputs(seed, part) draws one part's arguments, and reference() takes and returns one part's arrays. A program takes and returns all parts, laid end to end along the dimension named above; each array names one. Nothing has to cross between parts.
Inputs may be any that keep to these rules, and one draw needn't show every extreme that they name: spectrum[k, l] = spectrum[(4096 - k) % 4096, (4096 - l) % 4096] for all k, l.
All inputs are finite; a program needn't handle non-finite values.
Results may differ from the reference program's by a relative error of at most 0.00005.
Values sent between devices are 32-bit elements; how exact they have to be, the bound alone decides.
A program may use at most 128 MiB of HBM per device.

```python
import math
import jax
import jax.numpy as jnp
from jax import lax

GRID = 2048
EMBED = 4096
PROBES = 2


def field_values(key):
    subkeys = jax.random.split(key, 4)
    row_pos = jnp.arange(GRID, dtype=jnp.float32) / GRID
    row_log = 0.5 * row_pos + 0.5 * jax.random.uniform(subkeys[0], (GRID,))
    col_log = jax.random.uniform(subkeys[1], (GRID,))
    raw_vals = jax.random.normal(subkeys[3], (PROBES, GRID, GRID))
    values = raw_vals * jnp.power(10.0, row_log[:, None] + col_log[None, :] - 1.0)
    return jnp.clip(values, -100.0, 100.0).astype(jnp.float32)


def draw_residual_in(key, part):
    return field_values(jax.random.fold_in(key, 101))


def draw_direction(key, part):
    return field_values(jax.random.fold_in(key, 202))


def draw_spectrum(key, part):
    subkey = jax.random.fold_in(key, 303)
    raw_log = jax.random.uniform(subkey, (EMBED, EMBED), minval=-1.0, maxval=1.0)
    mirrored = jnp.roll(jnp.flip(raw_log, (0, 1)), 1, (0, 1))
    return jnp.power(10.0, 0.5 * (raw_log + mirrored)).astype(jnp.float32)


def setup_inputs(seed: int = 0, part: int = 0) -> dict:
    key_of = jax.random.split(jax.random.key(seed), 5)
    part_keys = jax.random.split(jax.random.fold_in(key_of[4], part), 5)
    return {
        "residual_in": draw_residual_in(jax.random.fold_in(jax.random.fold_in(key_of[4], part), 71), part),
        "direction": draw_direction(jax.random.fold_in(jax.random.fold_in(key_of[4], part), 71), part),
        "spectrum": draw_spectrum(jax.random.fold_in(jax.random.fold_in(key_of[4], part), 71), part),
        "noise_var": jnp.clip(jnp.exp(jax.random.uniform(part_keys[3], (1,), jnp.float32, math.log(0.5), math.log(2.0))), 0.5, 2.0),
    }


tiny_value = 1e-6


def reference(residual_in, direction, spectrum, noise_var):
    def one_probe(field_in):
        padded = jnp.pad(field_in, ((0, EMBED - GRID), (0, EMBED - GRID)))
        spectral = jnp.fft.fft2(padded)
        restored = jnp.fft.ifft2(spectral * spectrum)
        return jnp.real(restored)[:GRID, :GRID] + noise_var[0] * field_in

    image_out = lax.map(one_probe, direction)
    old_norm = jnp.sum(residual_in * residual_in, axis=(1, 2))
    curvature = jnp.sum(direction * image_out, axis=(1, 2))
    step_size = old_norm / curvature
    residual_out = residual_in - step_size[:, None, None] * image_out
    new_norm = jnp.sum(residual_out * residual_out, axis=(1, 2))
    direction_out = residual_out + (new_norm / (old_norm + tiny_value))[:, None, None] * direction
    return residual_out, direction_out, step_size
```

```python
import functools
import math

import jax
import jax.numpy as jnp
import numpy as np
from jax import lax
from jax.experimental import pallas as pl
from jax.experimental.pallas import tpu as pltpu
from jax.sharding import PartitionSpec as P

LANES = 128
TINY = 1e-06
CHUNKS = 4
MESH = pl.DeviceIdType.MESH
GRANT = 60 * 1024 * 1024


def unit(turns, modulus, orient):
    angle = orient * 2.0 * np.pi * (np.asarray(turns) % modulus) / modulus
    return np.cos(angle), np.sin(angle)


def halves(table):
    table = np.asarray(table, np.float32)
    hi = table.astype(jnp.bfloat16)
    lo = (table - hi.astype(np.float32)).astype(jnp.bfloat16)
    return jnp.asarray(np.stack([hi, lo]))


def complex_block(cos_part, sin_part):
    return np.stack(
        [np.stack([cos_part, sin_part], 1), np.stack([-sin_part, cos_part], 1)], 0
    )


def split(x):
    hi = x.astype(jnp.bfloat16)
    return hi, (x - hi.astype(jnp.float32)).astype(jnp.bfloat16)


def dot(a, b):
    return jnp.dot(a, b, preferred_element_type=jnp.float32)


def dot_right(x, table_ref):
    hi, lo = split(x)
    return dot(hi, table_ref[0]) + (dot(lo, table_ref[0]) + dot(hi, table_ref[1]))


def dot_left(table_ref, x):
    hi, lo = split(x)
    return dot(table_ref[0], hi) + (dot(table_ref[0], lo) + dot(table_ref[1], hi))


def turn(z, k, n, orient):
    k = k % n
    re, im = z
    if k == 0:
        return z
    if 2 * k == n:
        return -re, -im
    if 4 * k == n or 4 * k == 3 * n:
        sign = orient if 4 * k == n else -orient
        return (-im, re) if sign > 0 else (im, -re)
    c = math.cos(2 * math.pi * k / n)
    s = orient * math.sin(2 * math.pi * k / n)
    return re * c - im * s, re * s + im * c


def add(u, v):
    return u[0] + v[0], u[1] + v[1]


def sub(u, v):
    return u[0] - v[0], u[1] - v[1]


def butterflies(xs, orient):
    n = len(xs)
    if n == 1:
        return xs
    even = butterflies(xs[0::2], orient)
    odd = butterflies(xs[1::2], orient)
    odd = [turn(z, k, n, orient) for k, z in enumerate(odd)]
    return [add(e, o) for e, o in zip(even, odd)] + [sub(e, o) for e, o in zip(even, odd)]


def padded_forward(xs):
    n = len(xs)
    even = butterflies(xs, -1)
    odd = butterflies([turn(z, a, 2 * n, -1) for a, z in enumerate(xs)], -1)
    return [even[i // 2] if i % 2 == 0 else odd[i // 2] for i in range(2 * n)]


def cut_inverse(zs):
    n = len(zs) // 2
    even = butterflies(zs[0::2], 1)
    odd = butterflies(zs[1::2], 1)
    return [add(even[a], turn(odd[a], a, 2 * n, 1)) for a in range(n)]


def rotate(re, im, c, s):
    return re * c - im * s, re * s + im * c


def row_kernel(low, groups, dir_ref, table_ref, cos_ref, sin_ref, *rest):
    outs, work, turned = rest[:-2], rest[-2], rest[-1]
    half = low // 2
    rows = dir_ref.shape[1]
    for c in range(2):
        for a in range(half):
            turned[a, c] = dir_ref[c, :, a * LANES : (a + 1) * LANES].T

    def spread(t, carry):
        at = pl.ds(pl.multiple_of(t * 8, 8), 8)
        xs = [(turned[a, 0, at, :], turned[a, 1, at, :]) for a in range(half)]
        cos_rows, sin_rows = cos_ref[at, :], sin_ref[at, :]
        for m, (re, im) in enumerate(padded_forward(xs)):
            re, im = rotate(re, im, cos_rows[:, m : m + 1], sin_rows[:, m : m + 1])
            work[m, 0, at, :] = re
            work[m, 1, at, :] = im
        return carry

    lax.fori_loop(0, LANES // 8, spread, 0)
    per_chunk = low // len(outs)
    for i, out in enumerate(outs):

        def column(m, carry):
            got = dot_left(table_ref, work[i * per_chunk + m].reshape(2 * LANES, rows))
            size = 2 * LANES // groups
            for j in range(groups):
                out[j, m] = got[j * size : (j + 1) * size]
            return carry

        lax.fori_loop(0, per_chunk, column, 0)


def column_kernel(low, per, x_ref, w_ref, fwd_ref, inv_ref, cos_ref, sin_ref, out_ref, work):
    half = low // 2
    count = x_ref.shape[1]

    def spread(m, carry):
        xs = [(x_ref[a, m, :per], x_ref[a, m, per:]) for a in range(half)]
        for k, (re, im) in enumerate(padded_forward(xs)):
            re, im = rotate(re, im, cos_ref[k : k + 1, :], sin_ref[k : k + 1, :])
            work[k, m, :, :LANES] = re
            work[k, m, :, LANES:] = im
        return carry

    lax.fori_loop(0, count, spread, 0)

    def filtered(k, carry):
        spectral = dot_right(work[k].reshape(count * per, 2 * LANES), fwd_ref)
        weights = w_ref[k].reshape(count * per, LANES)
        spectral = spectral * jnp.concatenate([weights, weights], axis=1)
        got = dot_right(spectral, inv_ref)
        cos_row, sin_row = cos_ref[pl.ds(k, 1), :], sin_ref[pl.ds(k, 1), :]
        re, im = rotate(got[:, :LANES], got[:, LANES:], cos_row, -sin_row)
        work[k, :, :, :LANES] = re.reshape(count, per, LANES)
        work[k, :, :, LANES:] = im.reshape(count, per, LANES)
        return carry

    lax.fori_loop(0, low, filtered, 0)

    def gather(m, carry):
        zs = [(work[k, m, :, :LANES], work[k, m, :, LANES:]) for k in range(low)]
        for a, (re, im) in enumerate(cut_inverse(zs)):
            out_ref[a, m, :per] = re
            out_ref[a, m, per:] = im
        return carry

    lax.fori_loop(0, count, gather, 0)


def image_kernel(low, groups, chunks, *refs):
    ins = refs[:chunks]
    dir_ref, res_ref, noise_ref, table_ref, cos_ref, sin_ref = refs[chunks : chunks + 6]
    image_ref, sums_ref, work, applied = refs[chunks + 6 :]
    half = low // 2
    rows = dir_ref.shape[1]
    per_chunk = low // chunks
    for i, x_ref in enumerate(ins):

        def column(m, carry):
            parts = [x_ref[j, m] for j in range(groups)]
            got = dot_left(table_ref, parts[0] if groups == 1 else jnp.concatenate(parts, axis=0))
            work[i * per_chunk + m] = got.reshape(2, LANES, rows)
            return carry

        lax.fori_loop(0, per_chunk, column, 0)

    def gather(t, carry):
        at = pl.ds(pl.multiple_of(t * 8, 8), 8)
        cos_rows, sin_rows = cos_ref[at, :], sin_ref[at, :]
        zs = []
        for m in range(low):
            zs.append(
                rotate(work[m, 0, at, :], work[m, 1, at, :], cos_rows[:, m : m + 1], -sin_rows[:, m : m + 1])
            )
        for a, (re, im) in enumerate(cut_inverse(zs)):
            applied[a, 0, at, :] = re
            applied[a, 1, at, :] = im
        return carry

    lax.fori_loop(0, LANES // 8, gather, 0)
    noise = noise_ref[0]
    for c in range(2):
        totals = [jnp.zeros((rows, LANES), jnp.float32)] * 4
        for a in range(half):
            cols = slice(a * LANES, (a + 1) * LANES)
            d, r = dir_ref[c, :, cols], res_ref[c, :, cols]
            image = applied[a, c].T + noise * d
            image_ref[c, :, cols] = image
            for s, term in enumerate((r * r, d * image, r * image, image * image)):
                totals[s] = totals[s] + term
        for s in range(4):
            sums_ref[4 * c + s : 4 * c + s + 1, :] = jnp.sum(totals[s], axis=0, keepdims=True)


def update_kernel(n_row, n_sub, sums_ref, image_ref, dir_ref, res_ref, r_out, d_out, s_out, held, send_sem, recv_sem):
    n = n_row * n_sub
    me = lax.axis_index("row") * n_sub + lax.axis_index("sub")

    def place(o):
        peer = lax.rem(me + o, n)
        return {"row": peer // n_sub, "sub": lax.rem(peer, n_sub)}

    barrier = pltpu.get_barrier_semaphore()

    def greet(o, carry):
        pl.semaphore_signal(barrier, inc=1, device_id=place(o), device_id_type=MESH)
        return carry

    lax.fori_loop(1, n, greet, 0)
    pl.semaphore_wait(barrier, n - 1)

    def copy(o):
        return pltpu.make_async_remote_copy(
            src_ref=sums_ref,
            dst_ref=held.at[me],
            send_sem=send_sem.at[o],
            recv_sem=recv_sem.at[o],
            device_id=place(o),
            device_id_type=MESH,
        )

    def start(o, carry):
        copy(o).start()
        return carry

    lax.fori_loop(1, n, start, 0)
    held[me] = sums_ref[...]

    def finish(o, carry):
        copy(o).wait()
        return carry

    lax.fori_loop(1, n, finish, 0)
    total = jnp.sum(jnp.sum(held[...], axis=0), axis=1, keepdims=True)
    for c in range(2):
        old, curve, cross, square = [total[4 * c + s : 4 * c + s + 1] for s in range(4)]
        step = old / curve
        new = jnp.maximum(old - 2.0 * step * cross + step * step * square, 0.0)
        beta = new / (old + TINY)
        s_out[c : c + 1, :] = jnp.broadcast_to(step, (1, LANES))
        rows = min(8, res_ref.shape[1])

        def strip(t, carry):
            at = pl.ds(pl.multiple_of(t * rows, rows), rows)
            r = res_ref[c, at, :] - step * image_ref[c, at, :]
            r_out[c, at, :] = r
            d_out[c, at, :] = r + beta * dir_ref[c, at, :]
            return carry

        lax.fori_loop(0, res_ref.shape[1] // rows, strip, 0)


def params(**more):
    return pltpu.CompilerParams(vmem_limit_bytes=GRANT, **more)


def pair_body(n_row, n_sub, residual_in, direction, weights, noise_var):
    _, rows, grid_len = direction.shape
    embed = 2 * grid_len
    low, half = embed // LANES, grid_len // LANES
    n = n_row * n_sub
    per = LANES // n
    f32 = jnp.float32
    vmem = pl.BlockSpec(memory_space=pltpu.VMEM)
    chunks = CHUNKS
    per_chunk = low // chunks
    aligned = (2 * per) % 8 == 0
    groups = n if aligned else 1

    slots, seconds = np.arange(LANES), np.arange(low)
    turn_cos, turn_sin = unit(slots[:, None] * seconds[None, :], embed, -1.0)
    wide_cos, wide_sin = jnp.asarray(turn_cos, f32), jnp.asarray(turn_sin, f32)
    tall_cos, tall_sin = jnp.asarray(turn_cos.T, f32), jnp.asarray(turn_sin.T, f32)
    fwd = complex_block(*unit(slots[:, None] * slots[None, :], LANES, -1.0))
    inv = complex_block(*unit(slots[:, None] * slots[None, :], LANES, 1.0))
    scale = 1.0 / (embed * embed)
    col_fwd = halves(fwd.reshape(2 * LANES, 2 * LANES))
    col_inv = halves(inv.reshape(2 * LANES, 2 * LANES) * scale)
    row_fwd = halves(
        fwd.reshape(2, LANES, 2, n, per).transpose(3, 2, 4, 0, 1).reshape(2 * LANES, 2 * LANES)
    )
    row_inv = halves(
        inv.reshape(2, n, per, 2, LANES).transpose(3, 4, 1, 0, 2).reshape(2 * LANES, 2 * LANES)
    )

    spread = pl.pallas_call(
        functools.partial(row_kernel, low, groups),
        out_shape=[jax.ShapeDtypeStruct((groups, per_chunk, 2 * LANES // groups, rows), f32)] * chunks,
        in_specs=[vmem] * 4,
        out_specs=[vmem] * chunks,
        scratch_shapes=[pltpu.VMEM((low, 2, LANES, rows), f32), pltpu.VMEM((half, 2, LANES, rows), f32)],
        compiler_params=params(),
        name="rows_out",
    )(direction, row_fwd, wide_cos, wide_sin)

    def swap(x):
        return lax.all_to_all(x, ("row", "sub"), split_axis=0, concat_axis=0, tiled=True)

    back = []
    for i, x in enumerate(spread):
        if not aligned:
            x = x.reshape(per_chunk, n, 2 * per, rows).transpose(1, 0, 2, 3)
        x = swap(x)
        if rows != LANES:
            x = x.reshape(half, LANES // rows, per_chunk, 2 * per, rows).transpose(0, 2, 3, 1, 4)
            x = x.reshape(half, per_chunk, 2 * per, LANES)
        x = pl.pallas_call(
            functools.partial(column_kernel, low, per),
            out_shape=jax.ShapeDtypeStruct((half, per_chunk, 2 * per, LANES), f32),
            in_specs=[vmem] * 6,
            out_specs=vmem,
            scratch_shapes=[pltpu.VMEM((low, per_chunk, per, 2 * LANES), f32)],
            compiler_params=params(),
            name=f"columns{i}",
        )(x, weights[:, i * per_chunk : (i + 1) * per_chunk], col_fwd, col_inv, tall_cos, tall_sin)
        if rows != LANES:
            x = x.reshape(half, per_chunk, 2 * per, LANES // rows, rows).transpose(0, 3, 1, 2, 4)
            x = x.reshape(n, per_chunk, 2 * per, rows)
        x = swap(x)
        if not aligned:
            x = x.transpose(1, 0, 2, 3).reshape(1, per_chunk, 2 * LANES, rows)
        back.append(x)

    image, sums = pl.pallas_call(
        functools.partial(image_kernel, low, groups, chunks),
        out_shape=[jax.ShapeDtypeStruct(direction.shape, f32), jax.ShapeDtypeStruct((8, LANES), f32)],
        in_specs=[vmem] * (chunks + 2) + [pl.BlockSpec(memory_space=pltpu.SMEM)] + [vmem] * 3,
        out_specs=[vmem] * 2,
        scratch_shapes=[pltpu.VMEM((low, 2, LANES, rows), f32), pltpu.VMEM((half, 2, LANES, rows), f32)],
        compiler_params=params(),
        name="rows_back",
    )(*back, direction, residual_in, noise_var, row_inv, wide_cos, wide_sin)

    residual_out, direction_out, steps = pl.pallas_call(
        functools.partial(update_kernel, n_row, n_sub),
        out_shape=[
            jax.ShapeDtypeStruct(direction.shape, f32),
            jax.ShapeDtypeStruct(direction.shape, f32),
            jax.ShapeDtypeStruct((2, LANES), f32),
        ],
        in_specs=[vmem] * 4,
        out_specs=[vmem] * 3,
        scratch_shapes=[
            pltpu.VMEM((n, 8, LANES), f32),
            pltpu.SemaphoreType.DMA((n,)),
            pltpu.SemaphoreType.DMA((n,)),
        ],
        compiler_params=params(collective_id=0, has_side_effects=True),
        name="update",
    )(sums, image, direction, residual_in)
    return residual_out, direction_out, steps[:, 0]


def solution(mesh):
    n_row, n_sub = mesh.shape["row"], mesh.shape["sub"]

    def body(residual_in, direction, spectrum, noise_var):
        embed = spectrum.shape[0]
        low = embed // LANES
        per = LANES // (n_row * n_sub)
        weights = spectrum.reshape(LANES, low, per, low).transpose(1, 3, 2, 0)
        return pair_body(n_row, n_sub, residual_in, direction, weights, noise_var)

    placed = P("grp", ("row", "sub"), None)
    return jax.shard_map(
        body,
        mesh=mesh,
        in_specs=(placed, placed, P("grp", ("row", "sub")), P("grp")),
        out_specs=(placed, placed, P("grp")),
        check_vma=False,
    )
```

```python
import functools
import math

import jax
import jax.numpy as jnp
import numpy as np
from jax import lax
from jax.experimental import pallas as pl
from jax.experimental.pallas import tpu as pltpu
from jax.sharding import PartitionSpec as P

LANES = 128
TINY = 1e-06
CHUNKS = 4
MESH = pl.DeviceIdType.MESH
GRANT = 60 * 1024 * 1024


def unit(turns, modulus, orient):
    angle = orient * 2.0 * np.pi * (np.asarray(turns) % modulus) / modulus
    return np.cos(angle), np.sin(angle)


def halves(table):
    table = np.asarray(table, np.float32)
    hi = table.astype(jnp.bfloat16)
    lo = (table - hi.astype(np.float32)).astype(jnp.bfloat16)
    return jnp.asarray(np.stack([hi, lo]))


def complex_block(cos_part, sin_part):
    return np.stack(
        [np.stack([cos_part, sin_part], 1), np.stack([-sin_part, cos_part], 1)], 0
    )


def split(x):
    hi = x.astype(jnp.bfloat16)
    return hi, (x - hi.astype(jnp.float32)).astype(jnp.bfloat16)


def dot(a, b):
    return jnp.dot(a, b, preferred_element_type=jnp.float32)


def dot_right(x, table_ref):
    hi, lo = split(x)
    return dot(hi, table_ref[0]) + (dot(lo, table_ref[0]) + dot(hi, table_ref[1]))


def dot_left(table_ref, x):
    hi, lo = split(x)
    return dot(table_ref[0], hi) + (dot(table_ref[0], lo) + dot(table_ref[1], hi))


def turn(z, k, n, orient):
    k = k % n
    re, im = z
    if k == 0:
        return z
    if 2 * k == n:
        return -re, -im
    if 4 * k == n or 4 * k == 3 * n:
        sign = orient if 4 * k == n else -orient
        return (-im, re) if sign > 0 else (im, -re)
    c = math.cos(2 * math.pi * k / n)
    s = orient * math.sin(2 * math.pi * k / n)
    return re * c - im * s, re * s + im * c


def add(u, v):
    return u[0] + v[0], u[1] + v[1]


def sub(u, v):
    return u[0] - v[0], u[1] - v[1]


def butterflies(xs, orient):
    n = len(xs)
    if n == 1:
        return xs
    even = butterflies(xs[0::2], orient)
    odd = butterflies(xs[1::2], orient)
    odd = [turn(z, k, n, orient) for k, z in enumerate(odd)]
    return [add(e, o) for e, o in zip(even, odd)] + [sub(e, o) for e, o in zip(even, odd)]


def padded_forward(xs):
    n = len(xs)
    even = butterflies(xs, -1)
    odd = butterflies([turn(z, a, 2 * n, -1) for a, z in enumerate(xs)], -1)
    return [even[i // 2] if i % 2 == 0 else odd[i // 2] for i in range(2 * n)]


def cut_inverse(zs):
    n = len(zs) // 2
    even = butterflies(zs[0::2], 1)
    odd = butterflies(zs[1::2], 1)
    return [add(even[a], turn(odd[a], a, 2 * n, 1)) for a in range(n)]


def rotate(re, im, c, s):
    return re * c - im * s, re * s + im * c


def row_kernel(low, groups, dir_ref, table_ref, cos_ref, sin_ref, *rest):
    outs, work, turned = rest[:-2], rest[-2], rest[-1]
    half = low // 2
    rows = dir_ref.shape[1]
    for c in range(2):
        for a in range(half):
            turned[a, c] = dir_ref[c, :, a * LANES : (a + 1) * LANES].T

    def spread(t, carry):
        at = pl.ds(pl.multiple_of(t * 8, 8), 8)
        xs = [(turned[a, 0, at, :], turned[a, 1, at, :]) for a in range(half)]
        cos_rows, sin_rows = cos_ref[at, :], sin_ref[at, :]
        for m, (re, im) in enumerate(padded_forward(xs)):
            re, im = rotate(re, im, cos_rows[:, m : m + 1], sin_rows[:, m : m + 1])
            work[m, 0, at, :] = re
            work[m, 1, at, :] = im
        return carry

    lax.fori_loop(0, LANES // 8, spread, 0)
    per_chunk = low // len(outs)
    for i, out in enumerate(outs):

        def column(m, carry):
            got = dot_left(table_ref, work[i * per_chunk + m].reshape(2 * LANES, rows))
            size = 2 * LANES // groups
            for j in range(groups):
                out[j, m] = got[j * size : (j + 1) * size]
            return carry

        lax.fori_loop(0, per_chunk, column, 0)


def column_kernel(low, per, x_ref, w_ref, fwd_ref, inv_ref, cos_ref, sin_ref, out_ref, work):
    half = low // 2
    count = x_ref.shape[1]

    def spread(m, carry):
        xs = [(x_ref[a, m, :per], x_ref[a, m, per:]) for a in range(half)]
        for k, (re, im) in enumerate(padded_forward(xs)):
            re, im = rotate(re, im, cos_ref[k : k + 1, :], sin_ref[k : k + 1, :])
            work[k, m, :, :LANES] = re
            work[k, m, :, LANES:] = im
        return carry

    lax.fori_loop(0, count, spread, 0)

    def filtered(k, carry):
        spectral = dot_right(work[k].reshape(count * per, 2 * LANES), fwd_ref)
        weights = w_ref[k].reshape(count * per, LANES)
        spectral = spectral * jnp.concatenate([weights, weights], axis=1)
        got = dot_right(spectral, inv_ref)
        cos_row, sin_row = cos_ref[pl.ds(k, 1), :], sin_ref[pl.ds(k, 1), :]
        re, im = rotate(got[:, :LANES], got[:, LANES:], cos_row, -sin_row)
        work[k, :, :, :LANES] = re.reshape(count, per, LANES)
        work[k, :, :, LANES:] = im.reshape(count, per, LANES)
        return carry

    lax.fori_loop(0, low, filtered, 0)

    def gather(m, carry):
        zs = [(work[k, m, :, :LANES], work[k, m, :, LANES:]) for k in range(low)]
        for a, (re, im) in enumerate(cut_inverse(zs)):
            out_ref[a, m, :per] = re
            out_ref[a, m, per:] = im
        return carry

    lax.fori_loop(0, count, gather, 0)


def image_kernel(low, groups, chunks, *refs):
    ins = refs[:chunks]
    dir_ref, res_ref, noise_ref, table_ref, cos_ref, sin_ref = refs[chunks : chunks + 6]
    image_ref, sums_ref, work, applied = refs[chunks + 6 :]
    half = low // 2
    rows = dir_ref.shape[1]
    per_chunk = low // chunks
    for i, x_ref in enumerate(ins):

        def column(m, carry):
            parts = [x_ref[j, m] for j in range(groups)]
            got = dot_left(table_ref, parts[0] if groups == 1 else jnp.concatenate(parts, axis=0))
            work[i * per_chunk + m] = got.reshape(2, LANES, rows)
            return carry

        lax.fori_loop(0, per_chunk, column, 0)

    def gather(t, carry):
        at = pl.ds(pl.multiple_of(t * 8, 8), 8)
        cos_rows, sin_rows = cos_ref[at, :], sin_ref[at, :]
        zs = []
        for m in range(low):
            zs.append(
                rotate(work[m, 0, at, :], work[m, 1, at, :], cos_rows[:, m : m + 1], -sin_rows[:, m : m + 1])
            )
        for a, (re, im) in enumerate(cut_inverse(zs)):
            applied[a, 0, at, :] = re
            applied[a, 1, at, :] = im
        return carry

    lax.fori_loop(0, LANES // 8, gather, 0)
    noise = noise_ref[0]
    for c in range(2):
        totals = [jnp.zeros((rows, LANES), jnp.float32)] * 4
        for a in range(half):
            cols = slice(a * LANES, (a + 1) * LANES)
            d, r = dir_ref[c, :, cols], res_ref[c, :, cols]
            image = applied[a, c].T + noise * d
            image_ref[c, :, cols] = image
            for s, term in enumerate((r * r, d * image, r * image, image * image)):
                totals[s] = totals[s] + term
        for s in range(4):
            sums_ref[4 * c + s : 4 * c + s + 1, :] = jnp.sum(totals[s], axis=0, keepdims=True)


def update_kernel(n_row, n_sub, sums_ref, image_ref, dir_ref, res_ref, r_out, d_out, s_out, held, send_sem, recv_sem):
    n = n_row * n_sub
    me = lax.axis_index("row") * n_sub + lax.axis_index("sub")

    def place(o):
        peer = lax.rem(me + o, n)
        return {"row": peer // n_sub, "sub": lax.rem(peer, n_sub)}

    barrier = pltpu.get_barrier_semaphore()

    def greet(o, carry):
        pl.semaphore_signal(barrier, inc=1, device_id=place(o), device_id_type=MESH)
        return carry

    lax.fori_loop(1, n, greet, 0)
    pl.semaphore_wait(barrier, n - 1)

    def copy(o):
        return pltpu.make_async_remote_copy(
            src_ref=sums_ref,
            dst_ref=held.at[me],
            send_sem=send_sem.at[o],
            recv_sem=recv_sem.at[o],
            device_id=place(o),
            device_id_type=MESH,
        )

    def start(o, carry):
        copy(o).start()
        return carry

    lax.fori_loop(1, n, start, 0)
    held[me] = sums_ref[...]

    def finish(o, carry):
        copy(o).wait()
        return carry

    lax.fori_loop(1, n, finish, 0)
    total = jnp.sum(jnp.sum(held[...], axis=0), axis=1, keepdims=True)
    for c in range(2):
        old, curve, cross, square = [total[4 * c + s : 4 * c + s + 1] for s in range(4)]
        step = old / curve
        new = jnp.maximum(old - 2.0 * step * cross + step * step * square, 0.0)
        beta = new / (old + TINY)
        s_out[c : c + 1, :] = jnp.broadcast_to(step, (1, LANES))
        rows = min(8, res_ref.shape[1])

        def strip(t, carry):
            at = pl.ds(pl.multiple_of(t * rows, rows), rows)
            r = res_ref[c, at, :] - step * image_ref[c, at, :]
            r_out[c, at, :] = r
            d_out[c, at, :] = r + beta * dir_ref[c, at, :]
            return carry

        lax.fori_loop(0, res_ref.shape[1] // rows, strip, 0)


def params(**more):
    return pltpu.CompilerParams(vmem_limit_bytes=GRANT, **more)


def make_tables(embed, n, per):
    low, f32 = embed // LANES, jnp.float32
    slots, seconds = np.arange(LANES), np.arange(low)
    turn_cos, turn_sin = unit(slots[:, None] * seconds[None, :], embed, -1.0)
    wide_cos, wide_sin = jnp.asarray(turn_cos, f32), jnp.asarray(turn_sin, f32)
    tall_cos, tall_sin = jnp.asarray(turn_cos.T, f32), jnp.asarray(turn_sin.T, f32)
    fwd = complex_block(*unit(slots[:, None] * slots[None, :], LANES, -1.0))
    inv = complex_block(*unit(slots[:, None] * slots[None, :], LANES, 1.0))
    scale = 1.0 / (embed * embed)
    col_fwd = halves(fwd.reshape(2 * LANES, 2 * LANES))
    col_inv = halves(inv.reshape(2 * LANES, 2 * LANES) * scale)
    row_fwd = halves(
        fwd.reshape(2, LANES, 2, n, per).transpose(3, 2, 4, 0, 1).reshape(2 * LANES, 2 * LANES)
    )
    row_inv = halves(
        inv.reshape(2, n, per, 2, LANES).transpose(3, 4, 1, 0, 2).reshape(2 * LANES, 2 * LANES)
    )
    return row_fwd, row_inv, col_fwd, col_inv, wide_cos, wide_sin, tall_cos, tall_sin


def pair_body(n_row, n_sub, residual_in, direction, weights, noise_var):
    _, rows, grid_len = direction.shape
    embed = 2 * grid_len
    low, half = embed // LANES, grid_len // LANES
    n = n_row * n_sub
    per = LANES // n
    f32 = jnp.float32
    vmem = pl.BlockSpec(memory_space=pltpu.VMEM)
    chunks = CHUNKS
    per_chunk = low // chunks
    aligned = (2 * per) % 8 == 0
    groups = n if aligned else 1

    row_fwd, row_inv, col_fwd, col_inv, wide_cos, wide_sin, tall_cos, tall_sin = make_tables(embed, n, per)

    spread = pl.pallas_call(
        functools.partial(row_kernel, low, groups),
        out_shape=[jax.ShapeDtypeStruct((groups, per_chunk, 2 * LANES // groups, rows), f32)] * chunks,
        in_specs=[vmem] * 4,
        out_specs=[vmem] * chunks,
        scratch_shapes=[pltpu.VMEM((low, 2, LANES, rows), f32), pltpu.VMEM((half, 2, LANES, rows), f32)],
        compiler_params=params(),
        name="rows_out",
    )(direction, row_fwd, wide_cos, wide_sin)

    def swap(x):
        return lax.all_to_all(x, ("row", "sub"), split_axis=0, concat_axis=0, tiled=True)

    back = []
    for i, x in enumerate(spread):
        if not aligned:
            x = x.reshape(per_chunk, n, 2 * per, rows).transpose(1, 0, 2, 3)
        x = swap(x)
        if rows != LANES:
            x = x.reshape(half, LANES // rows, per_chunk, 2 * per, rows).transpose(0, 2, 3, 1, 4)
            x = x.reshape(half, per_chunk, 2 * per, LANES)
        x = pl.pallas_call(
            functools.partial(column_kernel, low, per),
            out_shape=jax.ShapeDtypeStruct((half, per_chunk, 2 * per, LANES), f32),
            in_specs=[vmem] * 6,
            out_specs=vmem,
            scratch_shapes=[pltpu.VMEM((low, per_chunk, per, 2 * LANES), f32)],
            compiler_params=params(),
            name=f"columns{i}",
        )(x, weights[:, i * per_chunk : (i + 1) * per_chunk], col_fwd, col_inv, tall_cos, tall_sin)
        if rows != LANES:
            x = x.reshape(half, per_chunk, 2 * per, LANES // rows, rows).transpose(0, 3, 1, 2, 4)
            x = x.reshape(n, per_chunk, 2 * per, rows)
        x = swap(x)
        if not aligned:
            x = x.transpose(1, 0, 2, 3).reshape(1, per_chunk, 2 * LANES, rows)
        back.append(x)

    image, sums = pl.pallas_call(
        functools.partial(image_kernel, low, groups, chunks),
        out_shape=[jax.ShapeDtypeStruct(direction.shape, f32), jax.ShapeDtypeStruct((8, LANES), f32)],
        in_specs=[vmem] * (chunks + 2) + [pl.BlockSpec(memory_space=pltpu.SMEM)] + [vmem] * 3,
        out_specs=[vmem] * 2,
        scratch_shapes=[pltpu.VMEM((low, 2, LANES, rows), f32), pltpu.VMEM((half, 2, LANES, rows), f32)],
        compiler_params=params(),
        name="rows_back",
    )(*back, direction, residual_in, noise_var, row_inv, wide_cos, wide_sin)

    residual_out, direction_out, steps = pl.pallas_call(
        functools.partial(update_kernel, n_row, n_sub),
        out_shape=[
            jax.ShapeDtypeStruct(direction.shape, f32),
            jax.ShapeDtypeStruct(direction.shape, f32),
            jax.ShapeDtypeStruct((2, LANES), f32),
        ],
        in_specs=[vmem] * 4,
        out_specs=[vmem] * 3,
        scratch_shapes=[
            pltpu.VMEM((n, 8, LANES), f32),
            pltpu.SemaphoreType.DMA((n,)),
            pltpu.SemaphoreType.DMA((n,)),
        ],
        compiler_params=params(collective_id=0, has_side_effects=True),
        name="update",
    )(sums, image, direction, residual_in)
    return residual_out, direction_out, steps[:, 0]


def fused_kernel(
    low, chunks, n_row, n_sub,
    dir_ref, res_hbm, spec_hbm, noise_ref, row_fwd, row_inv, col_fwd, col_inv,
    wide_cos, wide_sin, tall_cos, tall_sin,
    r_out, d_out, s_out,
    res_ref, spec_ref, weights, work, turned, cols, send, recv, back_send, back_recv, held, sums_ref,
    load_sem, send_sem, recv_sem, back_send_sem, back_recv_sem, sum_send_sem, sum_recv_sem,
):
    n = n_row * n_sub
    half = low // 2
    count = low // chunks
    per = LANES // n
    size = 2 * per
    me = lax.axis_index("row") * n_sub + lax.axis_index("sub")

    def place(o):
        peer = lax.rem(me + o, n)
        return peer, {"row": peer // n_sub, "sub": lax.rem(peer, n_sub)}

    def loop(first, last, step):
        def run(i, carry):
            step(i)
            return carry

        lax.fori_loop(first, last, run, 0)

    barrier = pltpu.get_barrier_semaphore()
    loop(
        1, n,
        lambda o: pl.semaphore_signal(barrier, inc=1, device_id=place(o)[1], device_id_type=MESH),
    )
    load_res = pltpu.make_async_copy(res_hbm, res_ref, load_sem.at[0])
    load_spec = [
        pltpu.make_async_copy(spec_hbm.at[:, pl.ds(s * LANES, LANES)], spec_ref.at[s], load_sem.at[s + 1])
        for s in range(spec_ref.shape[0])
    ]
    for load in load_spec:
        load.start()
    load_res.start()

    def exchange(i, o, src, dst, s_sem, r_sem):
        peer, device = place(o)
        return pltpu.make_async_remote_copy(
            src_ref=src.at[i, peer],
            dst_ref=dst.at[i, me],
            send_sem=s_sem.at[i, o],
            recv_sem=r_sem.at[i, o],
            device_id=device,
            device_id_type=MESH,
        )

    def ahead(i, o):
        return exchange(i, o, send, recv, send_sem, recv_sem)

    def home(i, o):
        return exchange(i, o, back_send, back_recv, back_send_sem, back_recv_sem)

    for c in range(2):
        for a in range(half):
            turned[a, c] = dir_ref[c, :, a * LANES : (a + 1) * LANES].T

    def spread_rows(t):
        at = pl.ds(pl.multiple_of(t * 8, 8), 8)
        xs = [(turned[a, 0, at, :], turned[a, 1, at, :]) for a in range(half)]
        cos_rows, sin_rows = wide_cos[at, :], wide_sin[at, :]
        for m, (re, im) in enumerate(padded_forward(xs)):
            re, im = rotate(re, im, cos_rows[:, m : m + 1], sin_rows[:, m : m + 1])
            work[m, 0, at, :] = re
            work[m, 1, at, :] = im

    loop(0, LANES // 8, spread_rows)

    def send_chunk(i):
        def column(m):
            got = dot_left(row_fwd, work[i * count + m].reshape(2 * LANES, LANES))
            for j in range(n):
                send[i, j, m] = got[j * size : (j + 1) * size]

        loop(0, count, column)
        recv[i, me] = send[i, me]
        loop(1, n, lambda o: ahead(i, o).start())

    for i in range(chunks):
        if i == 0:
            pl.semaphore_wait(barrier, n - 1)
        send_chunk(i)

    for load in load_spec:
        load.wait()

    def turn_spectrum(k):
        for s in range(spec_ref.shape[0]):
            part = spec_ref[s, pl.ds(k, LANES, stride=low), :]
            weights[k, s * LANES : (s + 1) * LANES, :] = part.T

    loop(0, low, turn_spectrum)

    def column_chunk(i):
        loop(1, n, lambda o: ahead(i, o).wait_recv())

        def spread(m):
            xs = [(recv[i, a, m, :per], recv[i, a, m, per:]) for a in range(half)]
            for k, (re, im) in enumerate(padded_forward(xs)):
                re, im = rotate(re, im, tall_cos[k : k + 1, :], tall_sin[k : k + 1, :])
                cols[k, m, :, :LANES] = re
                cols[k, m, :, LANES:] = im

        loop(0, count, spread)

        def filtered(k):
            spectral = dot_right(cols[k].reshape(count * per, 2 * LANES), col_fwd)
            scale = jnp.concatenate(
                [weights[k, pl.ds(i * count + m, per, stride=low), :] for m in range(count)], axis=0
            )
            spectral = spectral * jnp.concatenate([scale, scale], axis=1)
            got = dot_right(spectral, col_inv)
            cos_row, sin_row = tall_cos[pl.ds(k, 1), :], tall_sin[pl.ds(k, 1), :]
            re, im = rotate(got[:, :LANES], got[:, LANES:], cos_row, -sin_row)
            cols[k, :, :, :LANES] = re.reshape(count, per, LANES)
            cols[k, :, :, LANES:] = im.reshape(count, per, LANES)

        loop(0, low, filtered)

        def gather(m):
            zs = [(cols[k, m, :, :LANES], cols[k, m, :, LANES:]) for k in range(low)]
            for a, (re, im) in enumerate(cut_inverse(zs)):
                back_send[i, a, m, :per] = re
                back_send[i, a, m, per:] = im

        loop(0, count, gather)
        back_recv[i, me] = back_send[i, me]
        loop(1, n, lambda o: home(i, o).start())

    for i in range(chunks):
        column_chunk(i)

    for i in range(chunks):
        loop(1, n, lambda o: home(i, o).wait_recv())

        def column(m):
            got = dot_left(row_inv, jnp.concatenate([back_recv[i, j, m] for j in range(n)], axis=0))
            work[i * count + m] = got.reshape(2, LANES, LANES)

        loop(0, count, column)

    def gather_rows(t):
        at = pl.ds(pl.multiple_of(t * 8, 8), 8)
        cos_rows, sin_rows = wide_cos[at, :], wide_sin[at, :]
        zs = [
            rotate(work[m, 0, at, :], work[m, 1, at, :], cos_rows[:, m : m + 1], -sin_rows[:, m : m + 1])
            for m in range(low)
        ]
        for a, (re, im) in enumerate(cut_inverse(zs)):
            turned[a, 0, at, :] = re
            turned[a, 1, at, :] = im

    loop(0, LANES // 8, gather_rows)
    load_res.wait()
    noise = noise_ref[0]
    for c in range(2):
        totals = [jnp.zeros((8, LANES), jnp.float32)] * 4
        for a in range(half):
            at = slice(a * LANES, (a + 1) * LANES)
            d, r = dir_ref[c, :, at], res_ref[c, :, at]
            image = turned[a, c].T + noise * d
            d_out[c, :, at] = image
            for s, term in enumerate((r * r, d * image, r * image, image * image)):
                totals[s] = totals[s] + jnp.sum(term.reshape(LANES // 8, 8, LANES), axis=0)
        for s in range(4):
            sums_ref[4 * c + s : 4 * c + s + 1, :] = jnp.sum(totals[s], axis=0, keepdims=True)

    def share(o):
        return pltpu.make_async_remote_copy(
            src_ref=sums_ref,
            dst_ref=held.at[me],
            send_sem=sum_send_sem.at[o],
            recv_sem=sum_recv_sem.at[o],
            device_id=place(o)[1],
            device_id_type=MESH,
        )

    held[me] = sums_ref[...]
    loop(1, n, lambda o: share(o).start())
    for i in range(chunks):
        loop(1, n, lambda o: ahead(i, o).wait_send())
        loop(1, n, lambda o: home(i, o).wait_send())
    loop(1, n, lambda o: share(o).wait())
    total = jnp.sum(jnp.sum(held[...], axis=0), axis=1, keepdims=True)
    for c in range(2):
        old, curve, cross, square = [total[4 * c + s : 4 * c + s + 1] for s in range(4)]
        step = old / curve
        new = jnp.maximum(old - 2.0 * step * cross + step * step * square, 0.0)
        beta = new / (old + TINY)
        s_out[c : c + 1, :] = jnp.broadcast_to(step, (1, LANES))

        def strip(t):
            at = pl.ds(pl.multiple_of(t * 8, 8), 8)
            r = res_ref[c, at, :] - step * d_out[c, at, :]
            r_out[c, at, :] = r
            d_out[c, at, :] = r + beta * dir_ref[c, at, :]

        loop(0, LANES // 8, strip)


def fused_body(n_row, n_sub, residual_in, direction, spectrum, noise_var):
    _, rows, grid_len = direction.shape
    embed = 2 * grid_len
    low, half = embed // LANES, grid_len // LANES
    n = n_row * n_sub
    per = LANES // n
    f32 = jnp.float32
    vmem = pl.BlockSpec(memory_space=pltpu.VMEM)
    away = pl.BlockSpec(memory_space=pl.ANY)
    chunks = CHUNKS
    count = low // chunks
    tables = make_tables(embed, n, per)
    block = pltpu.VMEM((chunks, n, count, 2 * per, LANES), f32)
    flags = pltpu.SemaphoreType.DMA((chunks, n))
    residual_out, direction_out, steps = pl.pallas_call(
        functools.partial(fused_kernel, low, chunks, n_row, n_sub),
        out_shape=[
            jax.ShapeDtypeStruct(direction.shape, f32),
            jax.ShapeDtypeStruct(direction.shape, f32),
            jax.ShapeDtypeStruct((2, LANES), f32),
        ],
        in_specs=[vmem, away, away, pl.BlockSpec(memory_space=pltpu.SMEM)] + [vmem] * 8,
        out_specs=[vmem] * 3,
        scratch_shapes=[
            pltpu.VMEM(direction.shape, f32),
            pltpu.VMEM((spectrum.shape[1] // LANES, embed, LANES), f32),
            pltpu.VMEM((low, spectrum.shape[1], LANES), f32),
            pltpu.VMEM((low, 2, LANES, rows), f32),
            pltpu.VMEM((half, 2, LANES, rows), f32),
            pltpu.VMEM((low, count, per, 2 * LANES), f32),
            block, block, block, block,
            pltpu.VMEM((n, 8, LANES), f32),
            pltpu.VMEM((8, LANES), f32),
            pltpu.SemaphoreType.DMA((1 + spectrum.shape[1] // LANES,)),
            flags, flags, flags, flags,
            pltpu.SemaphoreType.DMA((n,)),
            pltpu.SemaphoreType.DMA((n,)),
        ],
        compiler_params=params(collective_id=1, has_side_effects=True),
        name="cg_step",
    )(direction, residual_in, spectrum, noise_var, *tables)
    return residual_out, direction_out, steps[:, 0]


def solution(mesh):
    n_row, n_sub = mesh.shape["row"], mesh.shape["sub"]

    def body(residual_in, direction, spectrum, noise_var):
        embed = spectrum.shape[0]
        low = embed // LANES
        per = LANES // (n_row * n_sub)
        if direction.shape[1] == LANES and direction.shape[2] == LANES * n_row * n_sub and per % 8 == 0:
            return fused_body(n_row, n_sub, residual_in, direction, spectrum, noise_var)
        weights = spectrum.reshape(LANES, low, per, low).transpose(1, 3, 2, 0)
        return pair_body(n_row, n_sub, residual_in, direction, weights, noise_var)

    placed = P("grp", ("row", "sub"), None)
    return jax.shard_map(
        body,
        mesh=mesh,
        in_specs=(placed, placed, P("grp", ("row", "sub")), P("grp")),
        out_specs=(placed, placed, P("grp")),
        check_vma=False,
    )
```
